32 devices in a mesh: row: 8 (over z, x), col: 2 (over y), rep: 2 (over core).
Axes of the slice: x: 2, y: 2, z: 4, core: 2. Of those that a mesh axis runs over, the one named last changes fastest.
Arguments:
- matrix: float32 [16384, 16384], P('row', 'col'), may hold values from -0.125 to 0.125
- vectors: float32 [64, 16384], P('rep', 'row'), may hold values from -0.3 to 0.3
Outputs:
- result: float32 [64, 16384], P('rep', 'row')
The draws below stay inside these ranges and needn't reach their ends.
All inputs are finite; a program needn't handle non-finite values.
Results may differ from the reference program's by a relative error of at most 0.00011.
Values sent between devices are 32-bit elements; how exact they have to be, the bound alone decides.
No kernel may reach another device: no remote copies, remote signals or barrier semaphores. Data moves between devices by JAX's collectives and lax.ppermute only.
A program may use at most 128 MiB of HBM per device.

```python
import jax
import jax.numpy as jnp
from jax import lax

N = 16384
COLS = 64
TERMS = 6
STEPS = 1


def block_scale(rng, dims, split, smallest, largest):
    factor_of = 1.0
    for position, blocks in split:
        steps = jax.random.uniform(jax.random.fold_in(jax.random.fold_in(rng, 6), position), (blocks,), jnp.float32, smallest / len(split), largest / len(split))
        factor_of = factor_of * jnp.repeat(jnp.exp(steps), dims[position] // blocks).reshape((-1,) + (1,) * (len(dims) - 1 - position))
    return factor_of


def gaussian(stream_key, shape, deviation, limit, pieces=(), dtype=jnp.bfloat16):
    factor_of = block_scale(stream_key, shape, pieces, -0.22, 0.18) if pieces else 1.0
    entries = jax.random.normal(stream_key, shape, jnp.float32) * deviation * factor_of
    return jnp.minimum(jnp.maximum(entries, -limit), limit).astype(dtype)


def setup_inputs(seed: int = 0) -> dict:
    key_list = jax.random.split(jax.random.key(seed), 3)
    matrix = gaussian(key_list[0], (N, N), (N // 7) ** -0.5, 0.125, ((0, 8), (1, 2)), jnp.float32)
    vectors = gaussian(key_list[1], (COLS, N), 0.05, 0.3, ((0, 2), (1, 8)), jnp.float32)
    return {"matrix": matrix, "vectors": vectors}


def reference(matrix, vectors):
    current = vectors
    for section in range(STEPS):
        summand = current
        running = current
        for degree in range(1, TERMS + 1):
            product = lax.dot_general(summand, matrix, (((1,), (1,)), ((), ())), precision=lax.Precision.HIGHEST, preferred_element_type=jnp.float32)
            summand = product / float(degree * STEPS)
            running = running + summand
        current = running
    return current
```

```python
import functools

import jax
import jax.numpy as jnp
from jax import lax
from jax.experimental import pallas as pl
from jax.experimental.pallas import tpu as pltpu
from jax.sharding import PartitionSpec as P


TERMS = 6
STEPS = 1
AXES = ("row", "col", "rep")
CHUNKS = 2
RING = 12


def split_kernel(fan, parts, matrix, *refs):
    outs, ring, sems = refs[: 2 * fan], refs[2 * fan], refs[2 * fan + 1]
    slots, step, depth = ring.shape
    rep, seat = lax.axis_index("rep"), lax.axis_index("row") % fan
    blocks = matrix.shape[0] // step
    each = blocks // parts
    total = fan * blocks
    tile = min(256, depth)
    shape = (tile, tile)
    diagonal = lax.broadcasted_iota(jnp.int32, shape, 0) == lax.broadcasted_iota(jnp.int32, shape, 1)
    identity = jnp.where(diagonal, 1.0, 0.0).astype(jnp.bfloat16)

    def copy(t):
        block = t % blocks
        row = pl.multiple_of(((rep ^ (block // each)) * each + block % each) * step, step)
        column = pl.multiple_of(((seat ^ (t // blocks)) * parts + rep) * depth, depth)
        slot = t % slots
        return pltpu.make_async_copy(
            matrix.at[pl.ds(row, step), pl.ds(column, depth)], ring.at[slot], sems.at[slot]
        )

    for t in range(min(slots, total)):
        copy(t).start()
    for q in range(fan):

        @pl.loop(0, blocks)
        def _(block, q=q):
            t = q * blocks + block
            copy(t).wait()
            value = ring[t % slots]
            top = value.astype(jnp.bfloat16)
            rest = (value - top.astype(jnp.float32)).astype(jnp.bfloat16)
            column = pl.multiple_of(block * step, step)
            for source, out in ((top, outs[2 * q]), (rest, outs[2 * q + 1])):
                for at in range(0, depth, tile):
                    turned = lax.dot_general(
                        identity,
                        source[:, at : at + tile],
                        (((1,), (1,)), ((), ())),
                        preferred_element_type=jnp.float32,
                    )
                    out[at : at + tile, pl.ds(column, step)] = turned.astype(jnp.bfloat16)

            @pl.when(t + slots < total)
            def _():
                copy(t + slots).start()


def split_matrix(matrix, fan, parts, depth):
    rows = matrix.shape[0]
    step = min(256, rows // parts)
    outs = pl.pallas_call(
        functools.partial(split_kernel, fan, parts),
        out_shape=(pltpu.VMEM((depth, rows), jnp.bfloat16),) * (2 * fan),
        in_specs=[pl.BlockSpec(memory_space=pl.ANY)],
        out_specs=(pl.BlockSpec(memory_space=pltpu.VMEM),) * (2 * fan),
        scratch_shapes=[
            pltpu.VMEM((RING, step, depth), jnp.float32),
            pltpu.SemaphoreType.DMA((RING,)),
        ],
        compiler_params=pltpu.CompilerParams(vmem_limit_bytes=20 << 20),
        cost_estimate=pl.CostEstimate(
            flops=8 * rows * depth * fan, bytes_accessed=4 * rows * depth * fan, transcendentals=0
        ),
        name="split",
    )(matrix)
    return list(zip(outs[::2], outs[1::2]))


def product_kernel(ranges, chunks, first, *refs):
    refs = list(refs)
    before = None if first else [refs.pop(0) for _ in ranges]
    value = jnp.concatenate([refs.pop(0)[...] for _ in range(chunks)], axis=1)
    upper, lower = refs.pop(0), refs.pop(0)
    count = value.shape[0]
    high = value.astype(jnp.bfloat16)
    low = (value - high.astype(jnp.float32)).astype(jnp.bfloat16)
    both = jnp.concatenate([high, low], axis=0)
    for place, (start, width) in enumerate(ranges):
        here = slice(start, start + width)
        main = jnp.dot(both, upper[:, here], preferred_element_type=jnp.float32)
        rest = jnp.dot(high, lower[:, here], preferred_element_type=jnp.float32)
        total = main[:count] + (main[count:] + rest)
        refs[place][...] = total if first else before[place][...] + total


def product(before, pieces, weights, ranges):
    count, depth = pieces[0].shape[0], weights[0].shape[0]
    width = sum(w for _, w in ranges)
    operands = list(before or []) + list(pieces) + list(weights)
    vmem = pl.BlockSpec(memory_space=pltpu.VMEM)
    return pl.pallas_call(
        functools.partial(product_kernel, ranges, len(pieces), before is None),
        out_shape=tuple(jax.ShapeDtypeStruct((count, w), jnp.float32) for _, w in ranges),
        in_specs=[vmem] * len(operands),
        out_specs=(vmem,) * len(ranges),
        input_output_aliases={} if before is None else {i: i for i in range(len(ranges))},
        compiler_params=pltpu.CompilerParams(vmem_limit_bytes=16 << 20),
        cost_estimate=pl.CostEstimate(
            flops=6 * count * depth * width,
            bytes_accessed=4 * depth * width,
            transcendentals=0,
        ),
        name="product",
    )(*operands)


def whole_call(kernel, outs, *operands):
    vmem = pl.BlockSpec(memory_space=pltpu.VMEM)
    return pl.pallas_call(
        kernel,
        out_shape=tuple(jax.ShapeDtypeStruct(shape, jnp.float32) for shape in outs),
        in_specs=[vmem] * len(operands),
        out_specs=(vmem,) * len(outs),
        compiler_params=pltpu.CompilerParams(vmem_limit_bytes=16 << 20),
    )(*operands)


def deal_kernel(vectors, *outs):
    rep = lax.axis_index("rep")
    width = outs[0].shape[1]
    for q, out in enumerate(outs):
        at = pl.multiple_of((rep ^ q) * width, width)
        out[...] = vectors[:, pl.ds(at, width)]


def sort_kernel(parts, *refs):
    rep = lax.axis_index("rep")
    values = [ref[...] for ref in refs[:parts]]
    size = values[0].shape[0]
    width = refs[parts].shape[1]
    for p in range(parts):
        value = values[0]
        for q in range(1, parts):
            value = jnp.where((rep ^ q) == p, values[q], value)
        for h, out in enumerate(refs[parts:]):
            out[p * size : (p + 1) * size, :] = value[:, h * width : (h + 1) * width]


def close_kernel(fan, parts, chunks, scale, *refs):
    count = parts * chunks
    sums, running, outs = refs[:count], refs[count : count + chunks], refs[count + chunks :]
    rep = lax.axis_index("rep")
    home = (lax.axis_index("row") // fan) == lax.axis_index("col")
    size, width = outs[0].shape[0], running[0].shape[1]
    for p in range(parts):
        for h in range(chunks):
            for v in range(parts):
                rows = slice(v * size, (v + 1) * size)
                value = sums[p * chunks + h][rows, :] * scale
                if p == 0:
                    value = value + jnp.where(home, running[h][rows, :], 0.0)
                at = pl.multiple_of((rep ^ p) * (width * chunks) + h * width, width)
                for q in range(parts):

                    @pl.when((rep ^ q) == v)
                    def _(value=value, out=outs[q], at=at):
                        out[:, pl.ds(at, width)] = value


def local(matrix, vectors):
    across, cols, parts = (lax.axis_size(axis) for axis in AXES)
    fan = across // cols
    count, rows = vectors.shape[0] * parts, vectors.shape[1]
    depth, size = rows // parts, vectors.shape[0]
    width = depth // CHUNKS

    def move(value, target):
        pairs = []
        for r in range(across):
            for c in range(cols):
                for k in range(parts):
                    h, s, d, e = target(r // fan, r % fan, c, k)
                    pairs.append(
                        ((r * cols + c) * parts + k, ((h * fan + s) * cols + d) * parts + e)
                    )
        return lax.ppermute(value, AXES, pairs)

    def swap_rep(value, q):
        return move(value, lambda h, s, c, k: (h, s, c, k ^ q))

    def swap_col(value, q):
        return move(value, lambda h, s, c, k: (h, s, c ^ q, k))

    def to_plane(value, q):
        return move(value, lambda h, s, c, k: ((c - q) % cols, s, h, k))

    def swap_seat(value, q):
        return move(value, lambda h, s, c, k: (h, s ^ q, c, k))

    slots = list(whole_call(deal_kernel, [(size, depth)] * parts, vectors))
    slots = [slots[0]] + [swap_rep(slots[q], q) for q in range(1, parts)]
    pieces = whole_call(functools.partial(sort_kernel, parts), [(count, width)] * CHUNKS, *slots)

    ranges = tuple((p * depth + h * width, width) for p in range(parts) for h in range(CHUNKS))
    running = None
    for degree in range(1, TERMS + 1):
        if degree == 1:
            own = [to_plane(piece, cols - 1) for piece in pieces]
            running = own
            weights = split_matrix(matrix, fan, parts, depth)
        else:
            own = []
            for piece in pieces:
                moved = [to_plane(piece, q) for q in reversed(range(cols))]
                own.append(sum(moved[1:], moved[0]) * scale)
            running = [a + b for a, b in zip(running, own)]
        groups = [own]
        for q in range(1, fan):
            groups.append([swap_seat(piece, q) for piece in own])
        sums = None
        for at in range(fan - 1):
            sums = product(sums, groups[at], weights[at], ranges)
        last = [None] * len(ranges)
        for h in range(CHUNKS):
            places = range(h, len(ranges), CHUNKS)
            done = product(
                None if sums is None else [sums[i] for i in places],
                groups[-1],
                weights[-1],
                tuple(ranges[i] for i in places),
            )
            for i, value in zip(places, done):
                last[i] = value
        sums = last
        scale = 1.0 / float(degree * STEPS)
        if degree < TERMS:
            pieces = []
            for h in range(CHUNKS):
                total = sums[h]
                for q in range(1, parts):
                    total = total + swap_rep(sums[q * CHUNKS + h], q)
                pieces.append(total)
    outs = whole_call(
        functools.partial(close_kernel, fan, parts, CHUNKS, scale),
        [(size, rows)] * parts,
        *sums,
        *running,
    )
    result = outs[0]
    for q in range(1, parts):
        result = result + swap_rep(outs[q], q)
    q = 1
    while q < cols:
        result = result + swap_col(result, q)
        q *= 2
    return result


def solution(mesh):
    placed = (P("row", "col"), P("rep", "row"))
    return jax.shard_map(
        local, mesh=mesh, in_specs=placed, out_specs=P("rep", "row"), check_vma=False
    )
```

```python
import functools

import jax
import jax.numpy as jnp
from jax import lax
from jax.experimental import pallas as pl
from jax.experimental.pallas import tpu as pltpu
from jax.sharding import PartitionSpec as P


TERMS = 6
STEPS = 1
AXES = ("row", "col", "rep")
CHUNKS = 2
RING = 8


def seat_order(fan, rep):
    order = list(range(1, fan))
    if rep % 2 and fan > 3:
        order[0], order[1] = order[1], order[0]
    return [0] + order


def split_kernel(fan, parts, matrix, *refs):
    outs, ring, sems = refs[: 2 * fan], refs[2 * fan], refs[2 * fan + 1]
    slots, step, depth = ring.shape
    rep, seat = lax.axis_index("rep"), lax.axis_index("row") % fan
    blocks = matrix.shape[0] // step
    each = blocks // parts
    total = fan * blocks
    tile = min(256, depth)
    shape = (tile, tile)
    diagonal = lax.broadcasted_iota(jnp.int32, shape, 0) == lax.broadcasted_iota(jnp.int32, shape, 1)
    identity = jnp.where(diagonal, 1.0, 0.0).astype(jnp.bfloat16)

    def copy(t):
        block = t % blocks
        row = pl.multiple_of(((rep ^ (block // each)) * each + block % each) * step, step)
        even, odd = 0, 0
        for q in range(fan):
            even = jnp.where(t // blocks == q, seat_order(fan, 0)[q], even)
            odd = jnp.where(t // blocks == q, seat_order(fan, 1)[q], odd)
        other = seat ^ jnp.where(rep % 2 == 0, even, odd)
        column = pl.multiple_of((other * parts + rep) * depth, depth)
        slot = t % slots
        return pltpu.make_async_copy(
            matrix.at[pl.ds(row, step), pl.ds(column, depth)], ring.at[slot], sems.at[slot]
        )

    for t in range(min(slots, total)):
        copy(t).start()
    for q in range(fan):

        @pl.loop(0, blocks)
        def _(block, q=q):
            t = q * blocks + block
            copy(t).wait()
            value = ring[t % slots]
            top = value.astype(jnp.bfloat16)
            rest = (value - top.astype(jnp.float32)).astype(jnp.bfloat16)
            column = pl.multiple_of(block * step, step)
            for at in range(0, depth, tile):
                turned = lax.dot_general(
                    identity,
                    top[:, at : at + tile],
                    (((1,), (1,)), ((), ())),
                    preferred_element_type=jnp.float32,
                )
                outs[2 * q][at : at + tile, pl.ds(column, step)] = turned.astype(jnp.bfloat16)
            outs[2 * q + 1][:, pl.ds(column, step)] = rest.T

            @pl.when(t + slots < total)
            def _():
                copy(t + slots).start()


def split_matrix(matrix, fan, parts, depth):
    rows = matrix.shape[0]
    step = min(256, rows // parts)
    outs = pl.pallas_call(
        functools.partial(split_kernel, fan, parts),
        out_shape=(pltpu.VMEM((depth, rows), jnp.bfloat16),) * (2 * fan),
        in_specs=[pl.BlockSpec(memory_space=pl.ANY)],
        out_specs=(pl.BlockSpec(memory_space=pltpu.VMEM),) * (2 * fan),
        scratch_shapes=[
            pltpu.VMEM((RING, step, depth), jnp.float32),
            pltpu.SemaphoreType.DMA((RING,)),
        ],
        compiler_params=pltpu.CompilerParams(vmem_limit_bytes=14 << 20),
        cost_estimate=pl.CostEstimate(
            flops=8 * rows * depth * fan, bytes_accessed=4 * rows * depth * fan, transcendentals=0
        ),
        name="split",
    )(matrix)
    return list(zip(outs[::2], outs[1::2]))


def product_kernel(ranges, terms, first, *refs):
    refs = list(refs)
    before = None if first else [refs.pop(0) for _ in ranges]
    sides = []
    for pieces, start in terms:
        value = jnp.concatenate([refs.pop(0)[...] for _ in range(pieces)], axis=1)
        high = value.astype(jnp.bfloat16)
        low = (value - high.astype(jnp.float32)).astype(jnp.bfloat16)
        both = jnp.concatenate([high, low], axis=0)
        sides.append((high, both, slice(start, start + value.shape[1])))
    weights = [(refs.pop(0), refs.pop(0)) for _ in terms]
    for place, (start, width) in enumerate(ranges):
        here = slice(start, start + width)
        total = None if first else before[place][...]
        for (high, both, rows), (upper, lower) in zip(sides, weights):
            count = high.shape[0]
            main = jnp.dot(both, upper[rows, here], preferred_element_type=jnp.float32)
            rest = jnp.dot(high, lower[rows, here], preferred_element_type=jnp.float32)
            value = main[:count] + (main[count:] + rest)
            total = value if total is None else total + value
        refs[place][...] = total


def product(before, terms, ranges):
    pieces = [piece for term in terms for piece in term[0]]
    weights = [part for term in terms for part in term[2]]
    count, chunk = pieces[0].shape
    width = sum(w for _, w in ranges)
    operands = list(before or []) + pieces + weights
    vmem = pl.BlockSpec(memory_space=pltpu.VMEM)
    shapes = tuple((len(term[0]), term[1] * chunk) for term in terms)
    return pl.pallas_call(
        functools.partial(product_kernel, ranges, shapes, before is None),
        out_shape=tuple(jax.ShapeDtypeStruct((count, w), jnp.float32) for _, w in ranges),
        in_specs=[vmem] * len(operands),
        out_specs=(vmem,) * len(ranges),
        input_output_aliases={} if before is None else {i: i for i in range(len(ranges))},
        compiler_params=pltpu.CompilerParams(vmem_limit_bytes=8 << 20),
        cost_estimate=pl.CostEstimate(
            flops=6 * count * chunk * len(pieces) * width,
            bytes_accessed=4 * chunk * len(pieces) * width,
            transcendentals=0,
        ),
        name="product",
    )(*operands)


def whole_call(kernel, outs, *operands):
    vmem = pl.BlockSpec(memory_space=pltpu.VMEM)
    return pl.pallas_call(
        kernel,
        out_shape=tuple(jax.ShapeDtypeStruct(shape, jnp.float32) for shape in outs),
        in_specs=[vmem] * len(operands),
        out_specs=(vmem,) * len(outs),
        compiler_params=pltpu.CompilerParams(vmem_limit_bytes=8 << 20),
    )(*operands)


def deal_kernel(vectors, *outs):
    rep = lax.axis_index("rep")
    width = outs[0].shape[1]
    for q, out in enumerate(outs):
        at = pl.multiple_of((rep ^ q) * width, width)
        out[...] = vectors[:, pl.ds(at, width)]


def sort_kernel(parts, *refs):
    rep = lax.axis_index("rep")
    values = [ref[...] for ref in refs[:parts]]
    size = values[0].shape[0]
    width = refs[parts].shape[1]
    for p in range(parts):
        value = values[0]
        for q in range(1, parts):
            value = jnp.where((rep ^ q) == p, values[q], value)
        for h, out in enumerate(refs[parts:]):
            out[p * size : (p + 1) * size, :] = value[:, h * width : (h + 1) * width]


def close_kernel(fan, parts, scale, *refs):
    sums, running, outs = refs[:parts], refs[parts], refs[parts + 1 :]
    rep = lax.axis_index("rep")
    home = (lax.axis_index("row") // fan) == lax.axis_index("col")
    size, width = outs[0].shape[0], running.shape[1]
    for p in range(parts):
        for v in range(parts):
            rows = slice(v * size, (v + 1) * size)
            value = sums[p][rows, :] * scale
            if p == 0:
                value = value + jnp.where(home, running[rows, :], 0.0)
            at = pl.multiple_of((rep ^ p) * width, width)
            for q in range(parts):

                @pl.when((rep ^ q) == v)
                def _(value=value, out=outs[q], at=at):
                    out[:, pl.ds(at, width)] = value


def local(matrix, vectors):
    across, cols, parts = (lax.axis_size(axis) for axis in AXES)
    fan = across // cols
    count, rows = vectors.shape[0] * parts, vectors.shape[1]
    depth, size = rows // parts, vectors.shape[0]
    width = depth // CHUNKS

    def move(value, target):
        pairs = []
        for r in range(across):
            for c in range(cols):
                for k in range(parts):
                    h, s, d, e = target(r // fan, r % fan, c, k)
                    pairs.append(
                        ((r * cols + c) * parts + k, ((h * fan + s) * cols + d) * parts + e)
                    )
        return lax.ppermute(value, AXES, pairs)

    def swap_rep(value, q):
        return move(value, lambda h, s, c, k: (h, s, c, k ^ q))

    def swap_col(value, q):
        return move(value, lambda h, s, c, k: (h, s, c ^ q, k))

    def to_plane(value, q):
        return move(value, lambda h, s, c, k: ((c - q) % cols, s, h, k))

    def swap_seat(value, q):
        return move(value, lambda h, s, c, k: (h, s ^ seat_order(fan, k)[q], c, k))

    slots = list(whole_call(deal_kernel, [(size, depth)] * parts, vectors))
    slots = [slots[0]] + [swap_rep(slots[q], q) for q in range(1, parts)]
    pieces = whole_call(functools.partial(sort_kernel, parts), [(count, width)] * CHUNKS, *slots)

    ranges = tuple((p * depth + h * width, width) for p in range(parts) for h in range(CHUNKS))
    running = None
    for degree in range(1, TERMS + 1):
        if degree == 1:
            own = [to_plane(piece, cols - 1) for piece in pieces]
            running = own
            weights = split_matrix(matrix, fan, parts, depth)
        else:
            own = []
            for piece in pieces:
                moved = [to_plane(piece, q) for q in reversed(range(cols))]
                own.append(sum(moved[1:], moved[0]) * scale)
            running = [a + b for a, b in zip(running, own)]
        groups = [own]
        for q in range(1, fan):
            groups.append([swap_seat(piece, q) for piece in own])
        sums = product(None, [(own, 0, weights[0])], ranges)
        for p in range(CHUNKS):
            some = [([groups[q][p]], p, weights[q]) for q in range(1, fan)]
            final = some.pop() if p == CHUNKS - 1 else None
            if some:
                sums = product(sums, some, ranges)
        last = [None] * len(ranges)
        for h in range(CHUNKS):
            places = range(h, len(ranges), CHUNKS)
            done = product([sums[i] for i in places], [final], tuple(ranges[i] for i in places))
            for i, value in zip(places, done):
                last[i] = value
        sums = last
        scale = 1.0 / float(degree * STEPS)
        if degree < TERMS:
            pieces = []
            for h in range(CHUNKS):
                total = sums[h]
                for q in range(1, parts):
                    total = total + swap_rep(sums[q * CHUNKS + h], q)
                pieces.append(total)
    pieces = []
    for h in range(CHUNKS):
        outs = whole_call(
            functools.partial(close_kernel, fan, parts, scale),
            [(size, parts * width)] * parts,
            *sums[h::CHUNKS],
            running[h],
        )
        result = outs[0]
        for q in range(1, parts):
            result = result + swap_rep(outs[q], q)
        q = 1
        while q < cols:
            result = result + swap_col(result, q)
            q *= 2
        pieces.append([result[:, p * width : (p + 1) * width] for p in range(parts)])
    return jnp.concatenate([pieces[h][p] for p in range(parts) for h in range(CHUNKS)], axis=1)


def solution(mesh):
    placed = (P("row", "col"), P("rep", "row"))
    return jax.shard_map(
        local, mesh=mesh, in_specs=placed, out_specs=P("rep", "row"), check_vma=False
    )
```

```python
import functools

import jax
import jax.numpy as jnp
from jax import lax
from jax.experimental import pallas as pl
from jax.experimental.pallas import tpu as pltpu
from jax.sharding import PartitionSpec as P


TERMS = 6
STEPS = 1
AXES = ("row", "col", "rep")
CHUNKS = 2
RING = 8
PAIR = 3
SHARE = 3
STEP = 512


def chunk_widths(depth):
    first = max(depth * SHARE // 8 // 128, 1) * 128
    return (first, depth - first)


def seat_order(fan, rep):
    order = list(range(1, fan))
    if rep % 2 and fan > 3:
        order[0], order[1] = order[1], order[0]
    return [0] + order


def split_kernel(fan, parts, matrix, *refs):
    outs, ring, sems = refs[: 2 * fan], refs[2 * fan], refs[2 * fan + 1]
    slots, step, depth = ring.shape
    rep, seat = lax.axis_index("rep"), lax.axis_index("row") % fan
    blocks = matrix.shape[0] // step
    each = blocks // parts
    total = fan * blocks
    tile = min(256, depth)
    shape = (tile, tile)
    diagonal = lax.broadcasted_iota(jnp.int32, shape, 0) == lax.broadcasted_iota(jnp.int32, shape, 1)
    identity = jnp.where(diagonal, 1.0, 0.0).astype(jnp.bfloat16)

    def copy(t):
        block = t % blocks
        row = pl.multiple_of(((rep ^ (block // each)) * each + block % each) * step, step)
        even, odd = 0, 0
        for q in range(fan):
            even = jnp.where(t // blocks == q, seat_order(fan, 0)[q], even)
            odd = jnp.where(t // blocks == q, seat_order(fan, 1)[q], odd)
        other = seat ^ jnp.where(rep % 2 == 0, even, odd)
        column = pl.multiple_of((other * parts + rep) * depth, depth)
        slot = t % slots
        return pltpu.make_async_copy(
            matrix.at[pl.ds(row, step), pl.ds(column, depth)], ring.at[slot], sems.at[slot]
        )

    for t in range(min(slots, total)):
        copy(t).start()
    for q in range(fan):

        @pl.loop(0, blocks)
        def _(block, q=q):
            t = q * blocks + block
            copy(t).wait()
            value = ring[t % slots]
            top = value.astype(jnp.bfloat16)
            rest = (value - top.astype(jnp.float32)).astype(jnp.bfloat16)
            column = pl.multiple_of(block * step, step)
            for at in range(0, depth, tile):
                turned = lax.dot_general(
                    identity,
                    top[:, at : at + tile],
                    (((1,), (1,)), ((), ())),
                    preferred_element_type=jnp.float32,
                )
                outs[2 * q][at : at + tile, pl.ds(column, step)] = turned.astype(jnp.bfloat16)
            outs[2 * q + 1][:, pl.ds(column, step)] = rest.T

            @pl.when(t + slots < total)
            def _():
                copy(t + slots).start()


def split_matrix(matrix, fan, parts, depth):
    rows = matrix.shape[0]
    step = min(256, rows // parts)
    outs = pl.pallas_call(
        functools.partial(split_kernel, fan, parts),
        out_shape=(pltpu.VMEM((depth, rows), jnp.bfloat16),) * (2 * fan),
        in_specs=[pl.BlockSpec(memory_space=pl.ANY)],
        out_specs=(pl.BlockSpec(memory_space=pltpu.VMEM),) * (2 * fan),
        scratch_shapes=[
            pltpu.VMEM((RING, step, depth), jnp.float32),
            pltpu.SemaphoreType.DMA((RING,)),
        ],
        compiler_params=pltpu.CompilerParams(vmem_limit_bytes=14 << 20),
        cost_estimate=pl.CostEstimate(
            flops=8 * rows * depth * fan, bytes_accessed=4 * rows * depth * fan, transcendentals=0
        ),
        name="split",
    )(matrix)
    return list(zip(outs[::2], outs[1::2]))


def product_kernel(ranges, terms, first, *refs):
    refs = list(refs)
    before = None if first else [refs.pop(0) for _ in ranges]
    sides = []
    for pieces, start in terms:
        value = jnp.concatenate([refs.pop(0)[...] for _ in range(pieces)], axis=1)
        high = value.astype(jnp.bfloat16)
        low = (value - high.astype(jnp.float32)).astype(jnp.bfloat16)
        both = jnp.concatenate([high, low], axis=0)
        sides.append((high, both, slice(start, start + value.shape[1])))
    weights = [(refs.pop(0), refs.pop(0)) for _ in terms]
    begin = 0
    while begin < len(ranges):
        end = begin + 1
        while end < len(ranges) and ranges[end][0] == sum(ranges[end - 1]):
            end += 1
        stop = sum(ranges[end - 1])
        for at in range(ranges[begin][0], stop, STEP):
            here = slice(at, min(at + STEP, stop))
            total = None
            for (high, both, rows), (upper, lower) in zip(sides, weights):
                count = high.shape[0]
                main = jnp.dot(both, upper[rows, here], preferred_element_type=jnp.float32)
                rest = jnp.dot(high, lower[rows, here], preferred_element_type=jnp.float32)
                value = main[:count] + (main[count:] + rest)
                total = value if total is None else total + value
            for place in range(begin, end):
                start, width = ranges[place]
                lo, hi = max(start, here.start), min(start + width, here.stop)
                if lo < hi:
                    value = total[:, lo - at : hi - at]
                    there = slice(lo - start, hi - start)
                    if not first:
                        value = before[place][:, there] + value
                    refs[place][:, there] = value
        begin = end


def product(before, terms, ranges):
    pieces = [piece for term in terms for piece in term[0]]
    weights = [part for term in terms for part in term[2]]
    count = pieces[0].shape[0]
    deep = sum(piece.shape[1] for piece in pieces)
    width = sum(w for _, w in ranges)
    operands = list(before or []) + pieces + weights
    vmem = pl.BlockSpec(memory_space=pltpu.VMEM)
    shapes = tuple((len(term[0]), term[1]) for term in terms)
    return pl.pallas_call(
        functools.partial(product_kernel, ranges, shapes, before is None),
        out_shape=tuple(jax.ShapeDtypeStruct((count, w), jnp.float32) for _, w in ranges),
        in_specs=[vmem] * len(operands),
        out_specs=(vmem,) * len(ranges),
        input_output_aliases={} if before is None else {i: i for i in range(len(ranges))},
        compiler_params=pltpu.CompilerParams(vmem_limit_bytes=8 << 20),
        cost_estimate=pl.CostEstimate(
            flops=6 * count * deep * width,
            bytes_accessed=4 * deep * width,
            transcendentals=0,
        ),
        name="product",
    )(*operands)


def whole_call(kernel, outs, *operands):
    vmem = pl.BlockSpec(memory_space=pltpu.VMEM)
    return pl.pallas_call(
        kernel,
        out_shape=tuple(jax.ShapeDtypeStruct(shape, jnp.float32) for shape in outs),
        in_specs=[vmem] * len(operands),
        out_specs=(vmem,) * len(outs),
        compiler_params=pltpu.CompilerParams(vmem_limit_bytes=8 << 20),
    )(*operands)


def deal_kernel(vectors, *outs):
    rep = lax.axis_index("rep")
    width = outs[0].shape[1]
    for q, out in enumerate(outs):
        at = pl.multiple_of((rep ^ q) * width, width)
        out[...] = vectors[:, pl.ds(at, width)]


def sort_kernel(parts, *refs):
    rep = lax.axis_index("rep")
    values = [ref[...] for ref in refs[:parts]]
    size = values[0].shape[0]
    for p in range(parts):
        value = values[0]
        for q in range(1, parts):
            value = jnp.where((rep ^ q) == p, values[q], value)
        at = 0
        for out in refs[parts:]:
            width = out.shape[1]
            out[p * size : (p + 1) * size, :] = value[:, at : at + width]
            at += width


def close_kernel(fan, parts, scale, *refs):
    sums, running, outs = refs[:parts], refs[parts], refs[parts + 1 :]
    rep = lax.axis_index("rep")
    home = (lax.axis_index("row") // fan) == lax.axis_index("col")
    size, width = outs[0].shape[0], running.shape[1]
    for p in range(parts):
        for v in range(parts):
            rows = slice(v * size, (v + 1) * size)
            value = sums[p][rows, :] * scale
            if p == 0:
                value = value + jnp.where(home, running[rows, :], 0.0)
            at = pl.multiple_of((rep ^ p) * width, width)
            for q in range(parts):

                @pl.when((rep ^ q) == v)
                def _(value=value, out=outs[q], at=at):
                    out[:, pl.ds(at, width)] = value


def local(matrix, vectors):
    across, cols, parts = (lax.axis_size(axis) for axis in AXES)
    fan = across // cols
    count, rows = vectors.shape[0] * parts, vectors.shape[1]
    depth, size = rows // parts, vectors.shape[0]
    widths = chunk_widths(depth)
    starts = [sum(widths[:h]) for h in range(CHUNKS)]

    def move(value, target):
        pairs = []
        for r in range(across):
            for c in range(cols):
                for k in range(parts):
                    h, s, d, e = target(r // fan, r % fan, c, k)
                    pairs.append(
                        ((r * cols + c) * parts + k, ((h * fan + s) * cols + d) * parts + e)
                    )
        return lax.ppermute(value, AXES, pairs)

    def swap_rep(value, q):
        return move(value, lambda h, s, c, k: (h, s, c, k ^ q))

    def swap_col(value, q):
        return move(value, lambda h, s, c, k: (h, s, c ^ q, k))

    def to_plane(value, q):
        return move(value, lambda h, s, c, k: ((c - q) % cols, s, h, k))

    def swap_seat(value, q):
        return move(value, lambda h, s, c, k: (h, s ^ seat_order(fan, k)[q], c, k))

    slots = list(whole_call(deal_kernel, [(size, depth)] * parts, vectors))
    slots = [slots[0]] + [swap_rep(slots[q], q) for q in range(1, parts)]
    pieces = whole_call(
        functools.partial(sort_kernel, parts), [(count, width) for width in widths], *slots
    )

    ranges = tuple(
        (p * depth + starts[h], widths[h]) for p in range(parts) for h in range(CHUNKS)
    )
    running = None
    for degree in range(1, TERMS + 1):
        if degree == 1:
            own = [to_plane(piece, cols - 1) for piece in pieces]
            running = own
            weights = split_matrix(matrix, fan, parts, depth)
        else:
            own = []
            for piece in pieces:
                moved = [to_plane(piece, q) for q in reversed(range(cols))]
                own.append(sum(moved[1:], moved[0]) * scale)
            running = [a + b for a, b in zip(running, own)]
        groups = [own]
        for q in range(1, fan):
            groups.append([swap_seat(piece, q) for piece in own])
        sums = product(None, [(own, 0, weights[0])], ranges)
        some = [([groups[q][p]], starts[p], weights[q]) for p in range(CHUNKS) for q in range(1, fan)]
        final = some.pop()
        for at in range(0, len(some), PAIR):
            sums = product(sums, some[at : at + PAIR], ranges)
        last = [None] * len(ranges)
        for h in range(CHUNKS):
            places = range(h, len(ranges), CHUNKS)
            done = product([sums[i] for i in places], [final], tuple(ranges[i] for i in places))
            for i, value in zip(places, done):
                last[i] = value
        sums = last
        scale = 1.0 / float(degree * STEPS)
        if degree < TERMS:
            pieces = []
            for h in range(CHUNKS):
                total = sums[h]
                for q in range(1, parts):
                    total = total + swap_rep(sums[q * CHUNKS + h], q)
                pieces.append(total)
    pieces = []
    for h, width in enumerate(widths):
        outs = whole_call(
            functools.partial(close_kernel, fan, parts, scale),
            [(size, parts * width)] * parts,
            *sums[h::CHUNKS],
            running[h],
        )
        result = outs[0]
        for q in range(1, parts):
            result = result + swap_rep(outs[q], q)
        q = 1
        while q < cols:
            result = result + swap_col(result, q)
            q *= 2
        pieces.append([result[:, p * width : (p + 1) * width] for p in range(parts)])
    return jnp.concatenate([pieces[h][p] for p in range(parts) for h in range(CHUNKS)], axis=1)


def solution(mesh):
    placed = (P("row", "col"), P("rep", "row"))
    return jax.shard_map(
        local, mesh=mesh, in_specs=placed, out_specs=P("rep", "row"), check_vma=False
    )
```
